32 devices in a mesh: groups: 2 (over y), aa: 4 (over z), ba: 2 (over x), col: 2 (over core).
Axes of the slice: x: 2, y: 2, z: 4, core: 2. Of those that a mesh axis runs over, the one named last changes fastest.
Arguments:
- hidden: bfloat16 [32, 128, 8192], P(('groups', 'aa'), None, ('ba', 'col')), parts along dimension 0, may hold values from -6 to 6
- key_value_weight: bfloat16 [2048, 8192], P('aa', ('ba', 'col')), may hold values from -0.09375 to 0.09375
- adapter_down_weight: bfloat16 [32, 32, 8192], P(('groups', 'aa'), None, ('ba', 'col')), parts along dimension 0, may hold values from -0.0625 to 0.0625
- adapter_up_weight: bfloat16 [32, 16, 2048], P(('groups', 'aa'), None, ('ba', 'col')), parts along dimension 0, may hold values from -1.5 to 1.5
- prompt_block_count: int32 [16], P('groups'), parts along dimension 0, may hold values from 1 to 3, 16 in all
- request_adapter: int32 [16], P('groups'), parts along dimension 0, may hold values from 0 to 15
- adapter_bank_row: int32 [32], P('groups'), parts along dimension 0, may hold values from 0 to 15, each once
Outputs:
- kv_states: bfloat16 [32, 128, 2048], P(('groups', 'aa'), None, ('ba', 'col')), parts along dimension 0
The draws below stay inside these ranges and needn't reach their ends.
There are 2 independent parts, one for each index of `groups`. The reference program is written for one: setup_inputs(seed, part) draws one part's arguments, and reference() takes and returns one part's arrays. A program takes and returns all parts, laid end to end along the dimension named above; an argument that names none is the same for every part. Nothing has to cross between parts.
Inputs may be any that keep to these rules, and one draw needn't show every extreme that they name: prompt_block_count sum to 16; some request has exactly 3 blocks. `adapter_bank_row`: each bank row holds one adapter; bank row s lies on index s // 4 of aa.
All inputs are finite; a program needn't handle non-finite values.
Results may differ from the reference program's by a relative error of at most 0.001.
Values may be sent and summed in bfloat16 or wider, within the bound.
A program may use at most 128 MiB of HBM per device.

```python
import math
import jax
import jax.numpy as jnp
import numpy as np
from jax import lax

MODEL_WIDTH = 8192
ADAPTER_RANK = 16
BLOCK = 128
MOSTC = 3
KEY_VALUE_WIDTH = 1024
BLOCKS = 16
REQS = 8
ADAPTER_COUNT = 16


def with_ends(array, key, smallest, top_value):
    shape = array.shape
    place = [jax.random.randint(jax.random.fold_in(key, axis), (), 0, shape[axis]) for axis in range(len(shape))]
    array = array.at[tuple(place)].set(smallest)
    longest = shape.index(max(shape))
    place[longest] = (place[longest] + 1) % shape[longest]
    return array.at[tuple(place)].set(top_value)


def with_spikes(entries, key, source, target, parts, factor):
    owner, partner = [(jnp.arange(entries.shape[axis_at]) // (entries.shape[axis_at] // parts)).reshape([-1 if axis == axis_at else 1 for axis in range(entries.ndim)]) for axis_at in (source, target)]
    chosen = jax.random.permutation(key, parts)[partner]
    strong = (owner == chosen) | (owner == (partner + parts // 2) % parts)
    return jnp.where(strong, factor * entries, entries)


def steps_of(own_key, shape, shards, low, top_value):
    loudness, own = 1.0, jax.random.fold_in(own_key, 6)
    for axis_at, parts in shards:
        heights = jnp.exp(jax.random.uniform(jax.random.fold_in(own, axis_at), (parts,), jnp.float32, low / len(shards), top_value / len(shards)))
        loudness = loudness * jnp.repeat(heights, shape[axis_at] // parts).reshape([-1 if axis == axis_at else 1 for axis in range(len(shape))])
    return loudness


def rank_table(count, skew):
    weights = [(1 << 20) // math.isqrt(standing ** skew) + 1 for standing in range(1, count + 1)]
    scale = 1 + sum(weights) // (1 << 30)
    return np.cumsum(np.array([max(1, weight // scale) for weight in weights]))


def ranked(stream_key, shape, count, skew):
    grid = rank_table(count, skew)
    lot = jax.random.randint(jax.random.fold_in(stream_key, 1), shape, 0, int(grid[count - 1]))
    standing = jnp.searchsorted(jnp.asarray(grid, jnp.int32), lot, side="right")
    return jax.random.permutation(jax.random.fold_in(stream_key, 2), count)[standing].astype(jnp.int32)


def length_profile(number_of, total, reach, lean):
    portions = [(1 << 20) // math.isqrt(standing ** lean) + 1 for standing in range(2, number_of + 1)]
    spare, holding = total - reach - (number_of - 1), [1] * (number_of - 1)
    while spare > 0:
        movable = [i for i in range(number_of - 1) if holding[i] < reach]
        pool, budget = sum([portions[i] for i in movable]), spare
        for i in movable:
            addition = min(reach - holding[i], max(1, budget * portions[i] // pool), spare)
            holding[i] = holding[i] + addition
            spare = spare - addition
    return np.array([reach] + holding)


def uneven(rng, count, total, bound, skew):
    if count == 2:
        one = jax.random.randint(rng, (), max(1, total - bound), min(bound, total - 1) + 1)
        return jnp.stack([one, total - one])
    lengths = jnp.asarray(length_profile(count, total, bound, skew), jnp.int32)
    pairs = (count - 1) // 2
    source_of, taker = lengths[1:1 + 2 * pairs:2], lengths[2:2 + 2 * pairs:2]
    slack = jnp.minimum(source_of - 1, bound - taker)
    shifted = jax.random.randint(jax.random.fold_in(rng, 1), (pairs,), 0, 1 << 20) % (slack + 1)
    lengths = lengths.at[1:1 + 2 * pairs:2].set(source_of - shifted).at[2:2 + 2 * pairs:2].set(taker + shifted)
    return lengths[jax.random.permutation(jax.random.fold_in(rng, 2), count)]


def scatter_about(key, extent, scale, most, shards=(), kind=jnp.bfloat16):
    entries = scale * jax.random.normal(key, extent, jnp.float32)
    if shards:
        entries = entries * steps_of(key, extent, shards, -0.22, 0.18)
    return jnp.clip(entries, -most, most).astype(kind)


def noise_with(stream_key, shape, scale, limit, pieces, heavy, kind=jnp.bfloat16):
    entries = scale * jax.random.normal(stream_key, shape, jnp.float32)
    if pieces:
        entries = entries * steps_of(stream_key, shape, pieces, -0.22, 0.18)
    return jnp.clip(with_spikes(entries, jax.random.fold_in(stream_key, 3), *heavy), -limit, limit).astype(kind)


def setup_inputs(seed: int = 0, part: int = 0) -> dict:
    seeds = jax.random.split(jax.random.key(seed), 8)
    part_keys = jax.random.split(jax.random.fold_in(seeds[7], part), 8)
    hidden = scatter_about(part_keys[0], (BLOCKS, BLOCK, MODEL_WIDTH), 1.0, 6.0, ((0, 4), (2, 4)))
    key_value_weight = noise_with(seeds[1], (2 * KEY_VALUE_WIDTH, MODEL_WIDTH), MODEL_WIDTH ** -0.5, 0.09375, ((0, 4), (1, 4)), (1, 0, 4, 2.0))
    adapter_down_weight = scatter_about(part_keys[2], (ADAPTER_COUNT, 2 * ADAPTER_RANK, MODEL_WIDTH), MODEL_WIDTH ** -0.5, 0.0625, ((0, 4), (2, 4)))
    adapter_up_weight = scatter_about(part_keys[3], (ADAPTER_COUNT, ADAPTER_RANK, 2 * KEY_VALUE_WIDTH), ADAPTER_RANK ** -0.5, 1.5, ((0, 4), (2, 4)))
    prompt_block_count = uneven(part_keys[4], REQS, BLOCKS, MOSTC, 2).astype(jnp.int32)
    request_adapter = with_ends(ranked(part_keys[5], (REQS,), ADAPTER_COUNT, 2), jax.random.fold_in(part_keys[5], 3), 0, ADAPTER_COUNT - 1).astype(jnp.int32)
    adapter_bank_row = jax.random.permutation(part_keys[6], ADAPTER_COUNT).astype(jnp.int32)
    return dict(hidden=hidden, key_value_weight=key_value_weight, adapter_down_weight=adapter_down_weight, adapter_up_weight=adapter_up_weight, prompt_block_count=prompt_block_count, request_adapter=request_adapter, adapter_bank_row=adapter_bank_row)


def block_slots(prompt_block_count, request_adapter, adapter_bank_row):
    block_ids = jnp.arange(BLOCKS, dtype=jnp.int32)
    block_ends = jnp.cumsum(prompt_block_count).astype(jnp.int32)
    request_of = jnp.sum((block_ends[None, :] <= block_ids[:, None]).astype(jnp.int32), axis=1).astype(jnp.int32)
    request_ids = jnp.arange(REQS, dtype=jnp.int32)
    adapter_of = jnp.sum(jnp.where(request_of[:, None] == request_ids[None, :], request_adapter[None, :], 0), axis=1).astype(jnp.int32)
    adapter_rows = jnp.arange(ADAPTER_COUNT, dtype=jnp.int32)
    return jnp.sum(jnp.where(adapter_of[:, None] == adapter_rows[None, :], adapter_bank_row[None, :], 0), axis=1).astype(jnp.int32)


def reference(hidden, key_value_weight, adapter_down_weight, adapter_up_weight, prompt_block_count, request_adapter, adapter_bank_row):
    bank_row_lookup = block_slots(prompt_block_count, request_adapter, adapter_bank_row)
    token_rows = hidden.reshape(BLOCKS * BLOCK, MODEL_WIDTH)
    base_output = lax.dot_general(token_rows, key_value_weight, (((1,), (1,)), ((), ())), preferred_element_type=jnp.float32)
    base_output = base_output.reshape(BLOCKS, BLOCK, 2 * KEY_VALUE_WIDTH)

    def single_block(operands):
        block_rows, current_bank_row = operands
        current_down_weight = lax.dynamic_index_in_dim(adapter_down_weight, current_bank_row, 0, keepdims=False)
        current_up_weight = lax.dynamic_index_in_dim(adapter_up_weight, current_bank_row, 0, keepdims=False).astype(jnp.float32)
        low_rank = lax.dot_general(block_rows, current_down_weight, (((1,), (1,)), ((), ())), preferred_element_type=jnp.float32)
        key_part = jnp.dot(low_rank[:, :ADAPTER_RANK], current_up_weight[:, :KEY_VALUE_WIDTH], precision=lax.Precision.HIGHEST)
        value_part = jnp.dot(low_rank[:, ADAPTER_RANK:], current_up_weight[:, KEY_VALUE_WIDTH:], precision=lax.Precision.HIGHEST)
        return jnp.concatenate([key_part, value_part], axis=1)

    adapter_output = lax.map(single_block, (hidden, bank_row_lookup))
    return (base_output + adapter_output).astype(jnp.bfloat16)
```

```python
import functools

import jax
import jax.numpy as jnp
from jax import lax
from jax.experimental import pallas as pl
from jax.experimental.pallas import tpu as pltpu
from jax.sharding import PartitionSpec as P

MESH = pl.DeviceIdType.MESH
PIECE = 32
NT = (((1,), (1,)), ((), ()))


def block_slots(prompt_block_count, request_adapter, adapter_bank_row, block_total):
    block_ids = jnp.arange(block_total, dtype=jnp.int32)
    block_ends = jnp.cumsum(prompt_block_count)
    request_of = jnp.sum((block_ends[None, :] <= block_ids[:, None]).astype(jnp.int32), axis=1)
    request_ids = jnp.arange(prompt_block_count.shape[0], dtype=jnp.int32)
    adapter_of = jnp.sum(
        jnp.where(request_of[:, None] == request_ids[None, :], request_adapter[None, :], 0), axis=1
    )
    adapter_rows = jnp.arange(adapter_bank_row.shape[0], dtype=jnp.int32)
    return jnp.sum(
        jnp.where(adapter_of[:, None] == adapter_rows[None, :], adapter_bank_row[None, :], 0),
        axis=1,
    )


def kernel(
    dims,
    hid_hbm, w_hbm, down_ref, up_ref, pd_ref, pu_ref,
    out_ref,
    hid, wbuf, sbuf, rbuf, lbuf, fin, lowbuf,
    load_sem, zrecv, yrecv, zsend, ysend, ssend, rrecv, lrecv, lsend, lowsend, lowrecv,
):
    n, groups, cols, shards, blocks, block_len, rank = dims
    chunk, feat = w_hbm.shape
    half = chunk // groups
    piece = min(PIECE, half)
    pieces = half // piece
    span = rbuf.shape[1]
    pair = 2 * rank
    down_rows = blocks * pair
    per_row = feat // span
    me = lax.axis_index("aa")
    group = lax.axis_index("groups")
    shard = lax.axis_index("ba") * cols + lax.axis_index("col")
    has_left, has_right = me > 0, me < n - 1

    def shard_id(j):
        return {"ba": j // cols, "col": j % cols}

    def other_shard(i):
        return lax.rem(shard + i, shards)

    def other_group(i):
        return lax.rem(group + i, groups)

    def remote(src, dst, send, recv, device_id):
        return pltpu.make_async_remote_copy(
            src_ref=src, dst_ref=dst, send_sem=send, recv_sem=recv,
            device_id=device_id, device_id_type=MESH,
        )

    load_w = pltpu.make_async_copy(w_hbm, wbuf.at[me], load_sem.at[0])
    load_h = pltpu.make_async_copy(hid_hbm, hid, load_sem.at[1])
    load_w.start()
    load_h.start()

    barrier = pltpu.get_barrier_semaphore()

    @pl.when(has_left)
    def _():
        pl.semaphore_signal(barrier, inc=1, device_id={"aa": me - 1}, device_id_type=MESH)

    @pl.when(has_right)
    def _():
        pl.semaphore_signal(barrier, inc=1, device_id={"aa": me + 1}, device_id_type=MESH)

    for i in range(1, groups):
        pl.semaphore_signal(
            barrier, inc=1, device_id={"groups": other_group(i)}, device_id_type=MESH
        )
    for i in range(1, shards):
        pl.semaphore_signal(
            barrier, inc=1, device_id=shard_id(other_shard(i)), device_id_type=MESH
        )
    greeted = jnp.where(has_left, 1, 0) + jnp.where(has_right, 1, 0) + groups + shards - 2
    pl.semaphore_wait(barrier, greeted)

    def along(way):
        return {"aa": me + (1 if way == 0 else -1)}

    def lora_copy(way, d):
        return remote(
            lbuf.at[way, d], lbuf.at[way, d], lsend.at[way, d], lrecv.at[way, d], along(way)
        )

    def add_own(d, write):
        tile = min(512, feat)
        for at in range(0, feat, tile):
            own = jnp.dot(
                pd_ref[d], down_ref[:, at:at + tile], preferred_element_type=jnp.float32
            )
            write(slice(0, down_rows), slice(at, at + tile), own)
        own = jnp.dot(pu_ref[d], up_ref[...], preferred_element_type=jnp.float32)
        for c in range(blocks):
            row = down_rows + (c // per_row) * rank
            at = (c % per_row) * span
            write(slice(row, row + rank), slice(at, at + span), own[c * rank:(c + 1) * rank])

    def lora_hop(way, d, valid, has_prev):
        @pl.when(valid)
        def _():
            @pl.when(has_prev)
            def _():
                lora_copy(way, d).wait_recv()

                def write(rows, at, own):
                    lbuf[way, d, rows, at] = (
                        lbuf[way, d, rows, at].astype(jnp.float32) + own
                    ).astype(jnp.bfloat16)

                add_own(d, write)

            @pl.when(jnp.logical_not(has_prev))
            def _():
                def write(rows, at, own):
                    lbuf[way, d, rows, at] = own.astype(jnp.bfloat16)

                add_own(d, write)

            lora_copy(way, d).start()

    def lora(r):
        turn = r - me
        d = n - 1 - turn
        lora_hop(0, d, jnp.logical_and(turn >= 0, d > me), has_left)
        turn = r - (n - 1 - me)
        lora_hop(1, turn, jnp.logical_and(turn >= 0, turn < me), has_right)

    def own_rows(p):
        return pl.ds(pl.multiple_of(group * half + p * piece, piece), piece)

    def z_copy(way, k, p, src=None):
        dst = wbuf.at[k, own_rows(p)]
        return remote(
            dst if src is None else src, dst, zsend.at[way, k], zrecv.at[k, p], along(way)
        )

    def y_copy(i, k, p):
        ref = wbuf.at[k, own_rows(p)]
        return remote(
            ref, ref, ysend.at[k, i], yrecv.at[k, p, i], {"groups": other_group(i)}
        )

    def forward(way, k, p):
        z_copy(way, k, p).wait_recv()

        @pl.when(has_right if way == 0 else has_left)
        def _():
            z_copy(way, k, p).start()

        for i in range(1, groups):
            y_copy(i, k, p).start()

    def product(k, row):
        row = pl.multiple_of(row, piece)
        got = lax.dot_general(
            wbuf[k, pl.ds(row, piece)], hid[...], NT, preferred_element_type=jnp.float32
        )
        column = k * chunk + row
        dest = column // span
        at = pl.ds(pl.multiple_of(column % span, piece), piece)

        @pl.when(dest == shard)
        def _():
            rbuf[shard, at] = got

        @pl.when(dest != shard)
        def _():
            sbuf[dest, at] = got
            remote(
                sbuf.at[dest, at], rbuf.at[shard, at], ssend.at[dest], rrecv.at[shard],
                shard_id(dest),
            ).start()

    def low_copy(i):
        j = other_shard(i)
        return remote(
            lowbuf.at[shard], lowbuf.at[shard], lowsend.at[i], lowrecv.at[shard], shard_id(j)
        )

    def low():
        def write(rows, at, own):
            fin[rows, at] = own.astype(jnp.bfloat16)

        add_own(me, write)
        for way, has_prev in ((0, has_left), (1, has_right)):
            @pl.when(has_prev)
            def _():
                remote(
                    lbuf.at[way, me], lbuf.at[way, me], lsend.at[way, me],
                    lrecv.at[way, me], along(1 - way),
                ).wait_recv()
                fin[...] = (
                    fin[...].astype(jnp.float32) + lbuf[way, me].astype(jnp.float32)
                ).astype(jnp.bfloat16)

        for c in range(blocks):
            lowbuf[shard, c * pair:(c + 1) * pair] = lax.dot_general(
                fin[c * pair:(c + 1) * pair], hid[c * block_len:(c + 1) * block_len], NT,
                preferred_element_type=jnp.float32,
            )
        for i in range(1, shards):
            low_copy(i).start()

    lora(0)
    for p in range(pieces):
        @pl.when(has_right)
        def _():
            z_copy(0, me, p, w_hbm.at[own_rows(p)]).start()

        @pl.when(has_left)
        def _():
            z_copy(1, me, p, w_hbm.at[own_rows(p)]).start()

    load_w.wait()
    load_h.wait()

    def step(s, carry):
        r, p = s // pieces, s % pieces

        @pl.when(jnp.logical_and(s < n * pieces, r > 0))
        def _():
            @pl.when(p == 0)
            def _():
                lora(r)

            @pl.when(s == (n - 1) * pieces)
            def _():
                low()

            @pl.when(me - r >= 0)
            def _():
                forward(0, me - r, p)

            @pl.when(me + r < n)
            def _():
                forward(1, me + r, p)

        @pl.when(s > 0)
        def _():
            r1, p1 = (s - 1) // pieces, (s - 1) % pieces

            def finish(k):
                product(k, group * half + p1 * piece)
                for i in range(1, groups):
                    g = other_group(groups - i)
                    row = g * half + p1 * piece
                    ref = wbuf.at[k, pl.ds(pl.multiple_of(row, piece), piece)]

                    @pl.when(k != me)
                    def _():
                        remote(
                            ref, ref, ysend.at[k, i], yrecv.at[k, p1, i], {"groups": g}
                        ).wait_recv()

                    product(k, row)

            @pl.when(me - r1 >= 0)
            def _():
                finish(me - r1)

            @pl.when(jnp.logical_and(r1 > 0, me + r1 < n))
            def _():
                finish(me + r1)

        return carry

    lax.fori_loop(0, n * pieces + 1, step, 0)

    for i in range(1, shards):
        j = other_shard(i)
        remote(
            lowbuf.at[j], lowbuf.at[j], lowsend.at[i], lowrecv.at[j], shard_id(j)
        ).wait_recv()
    for i in range(1, shards):
        j = other_shard(i)
        remote(rbuf.at[j], rbuf.at[j], ssend.at[j], rrecv.at[j], shard_id(j)).wait_recv()

    keys = shard < shards // 2
    for c in range(blocks):
        total = rbuf[0, :, c * block_len:(c + 1) * block_len]
        low_sum = lowbuf[0, c * pair:(c + 1) * pair]
        for j in range(1, shards):
            total = total + rbuf[j, :, c * block_len:(c + 1) * block_len]
            low_sum = low_sum + lowbuf[j, c * pair:(c + 1) * pair]
        active = jnp.where(keys, low_sum[:rank], low_sum[rank:])
        row = down_rows + (c // per_row) * rank
        at = (c % per_row) * span
        up = fin[row:row + rank, at:at + span].astype(jnp.float32)
        adapted = jnp.dot(
            active.T, up, precision=lax.Precision.HIGHEST, preferred_element_type=jnp.float32
        )
        out_ref[c * block_len:(c + 1) * block_len] = (total.T + adapted).astype(jnp.bfloat16)

    for k in range(n):
        part = wbuf.at[k, pl.ds(0, half)]
        for way, sent in (
            (0, jnp.logical_and(has_right, k <= me)),
            (1, jnp.logical_and(has_left, k >= me)),
        ):
            @pl.when(sent)
            def _():
                remote(
                    part, part, zsend.at[way, k], zrecv.at[k, 0], along(way)
                ).wait_send()

        @pl.when(k != me)
        def _():
            for i in range(1, groups):
                remote(
                    part, part, ysend.at[k, i], yrecv.at[k, 0, i], {"groups": other_group(i)}
                ).wait_send()

        @pl.when(k > me)
        def _():
            lora_copy(0, k).wait_send()

        @pl.when(k < me)
        def _():
            lora_copy(1, k).wait_send()

    for i in range(1, shards):
        j = other_shard(i)
        remote(sbuf.at[j], rbuf.at[shard], ssend.at[j], rrecv.at[shard], shard_id(j)).wait_send()
        low_copy(i).wait_send()


def body(
    sizes,
    hidden,
    key_value_weight,
    adapter_down_weight,
    adapter_up_weight,
    prompt_block_count,
    request_adapter,
    adapter_bank_row,
):
    n, groups, rows_x, cols = sizes
    shards = rows_x * cols
    blocks, block_len, feat = hidden.shape
    bank, pair, _ = adapter_down_weight.shape
    rank = pair // 2
    span = adapter_up_weight.shape[2]
    chunk = key_value_weight.shape[0]
    tokens = blocks * block_len
    half = chunk // groups
    pieces = half // min(PIECE, half)
    slots = block_slots(prompt_block_count, request_adapter, adapter_bank_row, blocks * n)
    owned = lax.axis_index("aa") * bank + jnp.arange(bank, dtype=jnp.int32)
    onehot = slots[:, None] == owned[None, :]

    def picker(width):
        same = jnp.arange(width)[:, None] == jnp.arange(width)[None, :]
        both = jnp.logical_and(onehot[:, None, :, None], same[None, :, None, :])
        return both.astype(jnp.bfloat16).reshape(n, blocks * width, bank * width)

    vmem = pl.BlockSpec(memory_space=pltpu.VMEM)
    hbm = pl.BlockSpec(memory_space=pl.ANY)
    low_rows = blocks * pair + blocks * rank * span // feat
    dma = pltpu.SemaphoreType.DMA
    out = pl.pallas_call(
        functools.partial(kernel, (n, groups, cols, shards, blocks, block_len, rank)),
        out_shape=jax.ShapeDtypeStruct((tokens, span), jnp.bfloat16),
        in_specs=[hbm, hbm, vmem, vmem, vmem, vmem],
        out_specs=vmem,
        scratch_shapes=[
            pltpu.VMEM((tokens, feat), jnp.bfloat16),
            pltpu.VMEM((n, chunk, feat), jnp.bfloat16),
            pltpu.VMEM((shards, span, tokens), jnp.float32),
            pltpu.VMEM((shards, span, tokens), jnp.float32),
            pltpu.VMEM((2, n, low_rows, feat), jnp.bfloat16),
            pltpu.VMEM((low_rows, feat), jnp.bfloat16),
            pltpu.VMEM((shards, blocks * pair, block_len), jnp.float32),
            dma((2,)),
            dma((n, pieces)),
            dma((n, pieces, groups)),
            dma((2, n)),
            dma((n, groups)),
            dma((shards,)),
            dma((shards,)),
            dma((2, n)),
            dma((2, n)),
            dma((shards,)),
            dma((shards,)),
        ],
        compiler_params=pltpu.CompilerParams(
            collective_id=0, has_side_effects=True, vmem_limit_bytes=60 * 1024 * 1024
        ),
    )(
        hidden.reshape(tokens, feat),
        key_value_weight,
        adapter_down_weight.reshape(bank * pair, feat),
        adapter_up_weight.reshape(bank * rank, span),
        picker(pair),
        picker(rank),
    )
    return out.reshape(blocks, block_len, span)


def solution(mesh):
    placed = (
        P(("groups", "aa"), None, ("ba", "col")),
        P("aa", ("ba", "col")),
        P(("groups", "aa"), None, ("ba", "col")),
        P(("groups", "aa"), None, ("ba", "col")),
        P("groups"),
        P("groups"),
        P("groups"),
    )
    sizes = tuple(mesh.shape[axis] for axis in ("aa", "groups", "ba", "col"))
    return jax.shard_map(
        functools.partial(body, sizes),
        mesh=mesh,
        in_specs=placed,
        out_specs=P(("groups", "aa"), None, ("ba", "col")),
        check_vma=False,
    )
```

```python
import functools

import jax
import jax.numpy as jnp
from jax import lax
from jax.experimental import pallas as pl
from jax.experimental.pallas import tpu as pltpu
from jax.sharding import PartitionSpec as P

MESH = pl.DeviceIdType.MESH
PIECE = 32
NT = (((1,), (1,)), ((), ()))


def block_slots(prompt_block_count, request_adapter, adapter_bank_row, block_total):
    block_ids = jnp.arange(block_total, dtype=jnp.int32)
    block_ends = jnp.cumsum(prompt_block_count)
    request_of = jnp.sum((block_ends[None, :] <= block_ids[:, None]).astype(jnp.int32), axis=1)
    request_ids = jnp.arange(prompt_block_count.shape[0], dtype=jnp.int32)
    adapter_of = jnp.sum(
        jnp.where(request_of[:, None] == request_ids[None, :], request_adapter[None, :], 0), axis=1
    )
    adapter_rows = jnp.arange(adapter_bank_row.shape[0], dtype=jnp.int32)
    return jnp.sum(
        jnp.where(adapter_of[:, None] == adapter_rows[None, :], adapter_bank_row[None, :], 0),
        axis=1,
    )


def kernel(
    dims,
    hid_hbm, w_hbm, down_ref, up_ref, pd_ref, pu_ref,
    out_ref,
    hid, wbuf, sbuf, rbuf, lbuf, fin, lowbuf,
    load_sem, zrecv, yrecv, zsend, ysend, ssend, rrecv, lrecv, lsend, lowsend, lowrecv,
):
    n, groups, cols, shards, blocks, block_len, rank = dims
    chunk, feat = w_hbm.shape
    half = chunk // groups
    piece = min(PIECE, half)
    pieces = half // piece
    span = rbuf.shape[1]
    pair = 2 * rank
    down_rows = blocks * pair
    per_row = feat // span
    me = lax.axis_index("aa")
    group = lax.axis_index("groups")
    shard = lax.axis_index("ba") * cols + lax.axis_index("col")
    has_left, has_right = me > 0, me < n - 1

    def shard_id(j):
        return {"ba": j // cols, "col": j % cols}

    def other_shard(i):
        return lax.rem(shard + i, shards)

    def other_group(i):
        return lax.rem(group + i, groups)

    def remote(src, dst, send, recv, device_id):
        return pltpu.make_async_remote_copy(
            src_ref=src, dst_ref=dst, send_sem=send, recv_sem=recv,
            device_id=device_id, device_id_type=MESH,
        )

    load_w = pltpu.make_async_copy(w_hbm, wbuf.at[me], load_sem.at[0])
    load_h = pltpu.make_async_copy(hid_hbm, hid, load_sem.at[1])
    load_w.start()
    load_h.start()

    barrier = pltpu.get_barrier_semaphore()

    @pl.when(has_left)
    def _():
        pl.semaphore_signal(barrier, inc=1, device_id={"aa": me - 1}, device_id_type=MESH)

    @pl.when(has_right)
    def _():
        pl.semaphore_signal(barrier, inc=1, device_id={"aa": me + 1}, device_id_type=MESH)

    for i in range(1, groups):
        pl.semaphore_signal(
            barrier, inc=1, device_id={"groups": other_group(i)}, device_id_type=MESH
        )
    for i in range(1, shards):
        pl.semaphore_signal(
            barrier, inc=1, device_id=shard_id(other_shard(i)), device_id_type=MESH
        )
    greeted = jnp.where(has_left, 1, 0) + jnp.where(has_right, 1, 0) + groups + shards - 2
    pl.semaphore_wait(barrier, greeted)

    def along(way):
        return {"aa": me + (1 if way == 0 else -1)}

    def lora_copy(way, d):
        return remote(
            lbuf.at[way, d], lbuf.at[way, d], lsend.at[way, d], lrecv.at[way, d], along(way)
        )

    def add_own(d, write):
        tile = min(512, feat)
        for at in range(0, feat, tile):
            own = jnp.dot(
                pd_ref[d], down_ref[:, at:at + tile], preferred_element_type=jnp.float32
            )
            write(slice(0, down_rows), slice(at, at + tile), own)
        own = jnp.dot(pu_ref[d], up_ref[...], preferred_element_type=jnp.float32)
        for c in range(blocks):
            row = down_rows + (c // per_row) * rank
            at = (c % per_row) * span
            write(slice(row, row + rank), slice(at, at + span), own[c * rank:(c + 1) * rank])

    def lora_hop(way, d, valid, has_prev):
        @pl.when(valid)
        def _():
            @pl.when(has_prev)
            def _():
                lora_copy(way, d).wait_recv()

                def write(rows, at, own):
                    lbuf[way, d, rows, at] = (
                        lbuf[way, d, rows, at].astype(jnp.float32) + own
                    ).astype(jnp.bfloat16)

                add_own(d, write)

            @pl.when(jnp.logical_not(has_prev))
            def _():
                def write(rows, at, own):
                    lbuf[way, d, rows, at] = own.astype(jnp.bfloat16)

                add_own(d, write)

            lora_copy(way, d).start()

    def lora(r):
        turn = r - me
        d = n - 1 - turn
        lora_hop(0, d, jnp.logical_and(turn >= 0, d > me), has_left)
        turn = r - (n - 1 - me)
        lora_hop(1, turn, jnp.logical_and(turn >= 0, turn < me), has_right)

    def own_rows(p):
        return pl.ds(pl.multiple_of(group * half + p * piece, piece), piece)

    def z_copy(way, k, p, src=None):
        dst = wbuf.at[k, own_rows(p)]
        return remote(
            dst if src is None else src, dst, zsend.at[way, k], zrecv.at[k, p], along(way)
        )

    def y_copy(i, k, p):
        ref = wbuf.at[k, own_rows(p)]
        return remote(
            ref, ref, ysend.at[k, i], yrecv.at[k, p, i], {"groups": other_group(i)}
        )

    def forward(way, k, p):
        z_copy(way, k, p).wait_recv()

        @pl.when(has_right if way == 0 else has_left)
        def _():
            z_copy(way, k, p).start()

        for i in range(1, groups):
            y_copy(i, k, p).start()

    def product(k, row):
        row = pl.multiple_of(row, piece)
        got = lax.dot_general(
            wbuf[k, pl.ds(row, piece)], hid[...], NT, preferred_element_type=jnp.float32
        )
        column = k * chunk + row
        dest = column // span
        at = pl.ds(pl.multiple_of(column % span, piece), piece)

        @pl.when(dest == shard)
        def _():
            rbuf[shard, at] = got

        @pl.when(dest != shard)
        def _():
            sbuf[dest, at] = got
            remote(
                sbuf.at[dest, at], rbuf.at[shard, at], ssend.at[dest], rrecv.at[shard],
                shard_id(dest),
            ).start()

    def low_copy(i):
        j = other_shard(i)
        return remote(
            lowbuf.at[shard], lowbuf.at[shard], lowsend.at[i], lowrecv.at[shard], shard_id(j)
        )

    def low():
        def write(rows, at, own):
            fin[rows, at] = own.astype(jnp.bfloat16)

        add_own(me, write)
        for way, has_prev in ((0, has_left), (1, has_right)):
            @pl.when(has_prev)
            def _():
                remote(
                    lbuf.at[way, me], lbuf.at[way, me], lsend.at[way, me],
                    lrecv.at[way, me], along(1 - way),
                ).wait_recv()
                fin[...] = (
                    fin[...].astype(jnp.float32) + lbuf[way, me].astype(jnp.float32)
                ).astype(jnp.bfloat16)

        for c in range(blocks):
            lowbuf[shard, c * pair:(c + 1) * pair] = lax.dot_general(
                fin[c * pair:(c + 1) * pair], hid[c * block_len:(c + 1) * block_len], NT,
                preferred_element_type=jnp.float32,
            )
        for i in range(1, shards):
            low_copy(i).start()

    lora(0)
    for p in range(pieces):
        @pl.when(has_right)
        def _():
            z_copy(0, me, p, w_hbm.at[own_rows(p)]).start()

        @pl.when(has_left)
        def _():
            z_copy(1, me, p, w_hbm.at[own_rows(p)]).start()

    load_w.wait()
    load_h.wait()

    def step(s, carry):
        r, p = s // pieces, s % pieces

        @pl.when(jnp.logical_and(s < n * pieces, r > 0))
        def _():
            @pl.when(p == 0)
            def _():
                lora(r)

            @pl.when(s == (n - 1) * pieces)
            def _():
                low()

            @pl.when(me - r >= 0)
            def _():
                forward(0, me - r, p)

            @pl.when(me + r < n)
            def _():
                forward(1, me + r, p)

        def compute(at):
            r1, p1 = at // pieces, at % pieces

            def finish(k):
                product(k, group * half + p1 * piece)
                for i in range(1, groups):
                    g = other_group(groups - i)
                    row = g * half + p1 * piece
                    ref = wbuf.at[k, pl.ds(pl.multiple_of(row, piece), piece)]

                    @pl.when(k != me)
                    def _():
                        remote(
                            ref, ref, ysend.at[k, i], yrecv.at[k, p1, i], {"groups": g}
                        ).wait_recv()

                    product(k, row)

            @pl.when(me - r1 >= 0)
            def _():
                finish(me - r1)

            @pl.when(jnp.logical_and(r1 > 0, me + r1 < n))
            def _():
                finish(me + r1)

        late = s - (n - 1) * pieces
        inner = jnp.logical_and(me > 0, me < n - 1)
        behind = (n - 2) * pieces + 2 * late

        @pl.when(jnp.logical_and(jnp.logical_not(inner), s > 0))
        def _():
            compute(s - 1)

        @pl.when(jnp.logical_and(inner, jnp.logical_and(late < 0, s >= pieces)))
        def _():
            compute(s - pieces)

        @pl.when(jnp.logical_and(inner, late > 0))
        def _():
            compute(behind - 1)

        @pl.when(jnp.logical_and(inner, jnp.logical_and(late >= 0, late < pieces)))
        def _():
            compute(behind)

        return carry

    lax.fori_loop(0, n * pieces + 1, step, 0)

    for i in range(1, shards):
        j = other_shard(i)
        remote(
            lowbuf.at[j], lowbuf.at[j], lowsend.at[i], lowrecv.at[j], shard_id(j)
        ).wait_recv()
    for i in range(1, shards):
        j = other_shard(i)
        remote(rbuf.at[j], rbuf.at[j], ssend.at[j], rrecv.at[j], shard_id(j)).wait_recv()

    keys = shard < shards // 2
    for c in range(blocks):
        total = rbuf[0, :, c * block_len:(c + 1) * block_len]
        low_sum = lowbuf[0, c * pair:(c + 1) * pair]
        for j in range(1, shards):
            total = total + rbuf[j, :, c * block_len:(c + 1) * block_len]
            low_sum = low_sum + lowbuf[j, c * pair:(c + 1) * pair]
        active = jnp.where(keys, low_sum[:rank], low_sum[rank:])
        row = down_rows + (c // per_row) * rank
        at = (c % per_row) * span
        up = fin[row:row + rank, at:at + span].astype(jnp.float32)
        adapted = jnp.dot(
            active.T, up, precision=lax.Precision.HIGHEST, preferred_element_type=jnp.float32
        )
        out_ref[c * block_len:(c + 1) * block_len] = (total.T + adapted).astype(jnp.bfloat16)

    for k in range(n):
        part = wbuf.at[k, pl.ds(0, half)]
        for way, sent in (
            (0, jnp.logical_and(has_right, k <= me)),
            (1, jnp.logical_and(has_left, k >= me)),
        ):
            @pl.when(sent)
            def _():
                remote(
                    part, part, zsend.at[way, k], zrecv.at[k, 0], along(way)
                ).wait_send()

        @pl.when(k != me)
        def _():
            for i in range(1, groups):
                remote(
                    part, part, ysend.at[k, i], yrecv.at[k, 0, i], {"groups": other_group(i)}
                ).wait_send()

        @pl.when(k > me)
        def _():
            lora_copy(0, k).wait_send()

        @pl.when(k < me)
        def _():
            lora_copy(1, k).wait_send()

    for i in range(1, shards):
        j = other_shard(i)
        remote(sbuf.at[j], rbuf.at[shard], ssend.at[j], rrecv.at[shard], shard_id(j)).wait_send()
        low_copy(i).wait_send()


def body(
    sizes,
    hidden,
    key_value_weight,
    adapter_down_weight,
    adapter_up_weight,
    prompt_block_count,
    request_adapter,
    adapter_bank_row,
):
    n, groups, rows_x, cols = sizes
    shards = rows_x * cols
    blocks, block_len, feat = hidden.shape
    bank, pair, _ = adapter_down_weight.shape
    rank = pair // 2
    span = adapter_up_weight.shape[2]
    chunk = key_value_weight.shape[0]
    tokens = blocks * block_len
    half = chunk // groups
    pieces = half // min(PIECE, half)
    slots = block_slots(prompt_block_count, request_adapter, adapter_bank_row, blocks * n)
    owned = lax.axis_index("aa") * bank + jnp.arange(bank, dtype=jnp.int32)
    onehot = slots[:, None] == owned[None, :]

    def picker(width):
        same = jnp.arange(width)[:, None] == jnp.arange(width)[None, :]
        both = jnp.logical_and(onehot[:, None, :, None], same[None, :, None, :])
        return both.astype(jnp.bfloat16).reshape(n, blocks * width, bank * width)

    vmem = pl.BlockSpec(memory_space=pltpu.VMEM)
    hbm = pl.BlockSpec(memory_space=pl.ANY)
    low_rows = blocks * pair + blocks * rank * span // feat
    dma = pltpu.SemaphoreType.DMA
    out = pl.pallas_call(
        functools.partial(kernel, (n, groups, cols, shards, blocks, block_len, rank)),
        out_shape=jax.ShapeDtypeStruct((tokens, span), jnp.bfloat16),
        in_specs=[hbm, hbm, vmem, vmem, vmem, vmem],
        out_specs=vmem,
        scratch_shapes=[
            pltpu.VMEM((tokens, feat), jnp.bfloat16),
            pltpu.VMEM((n, chunk, feat), jnp.bfloat16),
            pltpu.VMEM((shards, span, tokens), jnp.float32),
            pltpu.VMEM((shards, span, tokens), jnp.float32),
            pltpu.VMEM((2, n, low_rows, feat), jnp.bfloat16),
            pltpu.VMEM((low_rows, feat), jnp.bfloat16),
            pltpu.VMEM((shards, blocks * pair, block_len), jnp.float32),
            dma((2,)),
            dma((n, pieces)),
            dma((n, pieces, groups)),
            dma((2, n)),
            dma((n, groups)),
            dma((shards,)),
            dma((shards,)),
            dma((2, n)),
            dma((2, n)),
            dma((shards,)),
            dma((shards,)),
        ],
        compiler_params=pltpu.CompilerParams(
            collective_id=0, has_side_effects=True, vmem_limit_bytes=60 * 1024 * 1024
        ),
    )(
        hidden.reshape(tokens, feat),
        key_value_weight,
        adapter_down_weight.reshape(bank * pair, feat),
        adapter_up_weight.reshape(bank * rank, span),
        picker(pair),
        picker(rank),
    )
    return out.reshape(blocks, block_len, span)


def solution(mesh):
    placed = (
        P(("groups", "aa"), None, ("ba", "col")),
        P("aa", ("ba", "col")),
        P(("groups", "aa"), None, ("ba", "col")),
        P(("groups", "aa"), None, ("ba", "col")),
        P("groups"),
        P("groups"),
        P("groups"),
    )
    sizes = tuple(mesh.shape[axis] for axis in ("aa", "groups", "ba", "col"))
    return jax.shard_map(
        functools.partial(body, sizes),
        mesh=mesh,
        in_specs=placed,
        out_specs=P(("groups", "aa"), None, ("ba", "col")),
        check_vma=False,
    )
```
